32 devices in a mesh: gx: 16 (over z, x, core), gy: 2 (over y).
Axes of the slice: x: 2, y: 2, z: 4, core: 2. Of those that a mesh axis runs over, the one named last changes fastest.
Arguments:
- prefix_tokens: bfloat16 [12288, 8192], P('gx'), may hold values from -6 to 6
- key_value_weight: bfloat16 [8192, 2048], P('gx', 'gy'), may hold values from -0.0625 to 0.0625
- prefix_lengths: int32 [96], P('gx'), may hold values from 1 to 128, as said below
- start_offsets: int32 [96], P('gx'), may hold values from 0 to 1920
- queries: bfloat16 [4, 8192], P('gy'), may hold values from -5 to 5
- key_value_cache: bfloat16 [2, 4, 2048, 1024], P(None, 'gy', 'gx'), may hold values from -5 to 5
- cache_lengths: int32 [4], P('gy'), may hold values from 256 to 2048, as said below
- out_weight: bfloat16 [8192, 8192], P('gy', 'gx'), may hold values from -0.5 to 0.5
Outputs:
- prefix_kv: bfloat16 [12288, 2048], P('gx', 'gy')
- decode_out: bfloat16 [4, 8192], P('gy', 'gx')
The draws below stay inside these ranges and needn't reach their ends.
Inputs may be any that keep to these rules, and one draw needn't show every extreme that they name: `prefix_lengths`: live tokens stand at the front of a prefix's slots; in every draw some prefix uses all 128 slots. `cache_lengths`: live positions stand at the front of a trajectory's cache; in every draw some trajectory uses all 2048 positions.
All inputs are finite; a program needn't handle non-finite values.
Results may differ from the reference program's by a relative error of at most 0.0051.
Values may be sent and summed in bfloat16 or wider, within the bound.
A program may use at most 64 MiB of HBM per device.

```python
import jax
import jax.numpy as jnp
from jax import lax

MODEL_WIDTH = 8192
QUERY_HEADS = 64
KEY_VALUE_HEADS = 8
HEAD_SIZE = 128
SLOT = 128
CACHE_PER_SHARD = 128
SEQS = 96
TOKENS = 12288
TRAJECTORY_COUNT = 4
CACHE_LENGTH = 2048
N_GX = 16


def draw_queries(key, part):
    base_key = jax.random.fold_in(key, 21)
    value_rows = jnp.clip(2.0 * jax.random.normal(base_key, (TRAJECTORY_COUNT, QUERY_HEADS * HEAD_SIZE), jnp.float32), -5.0, 5.0)
    return value_rows.astype(jnp.bfloat16)


def draw_key_value_cache(key, part):
    base_key = jax.random.fold_in(key, 22)
    array_shape = (2, TRAJECTORY_COUNT, CACHE_LENGTH, KEY_VALUE_HEADS * HEAD_SIZE)
    value_rows = jnp.clip(jax.random.normal(base_key, array_shape, jnp.float32), -5.0, 5.0)
    return value_rows.astype(jnp.bfloat16)


def draw_cache_lengths(key, part):
    lengths = jax.random.randint(jax.random.fold_in(key, 31), (TRAJECTORY_COUNT,), CACHE_LENGTH // 8, CACHE_LENGTH + 1)
    full_index = jax.random.randint(jax.random.fold_in(key, 32), (), 0, TRAJECTORY_COUNT)
    short_value = jax.random.randint(jax.random.fold_in(key, 33), (), CACHE_LENGTH // 8, CACHE_LENGTH)
    lengths = lengths.at[(full_index + 1) % TRAJECTORY_COUNT].set(short_value)
    return lengths.at[full_index].set(CACHE_LENGTH).astype(jnp.int32)


def draw_prefix_lengths(key, part):
    lengths = jax.random.randint(jax.random.fold_in(key, 41), (SEQS,), 1, SLOT + 1)
    full_index = jax.random.randint(jax.random.fold_in(key, 42), (), 0, SEQS)
    short_value = jax.random.randint(jax.random.fold_in(key, 43), (), 1, SLOT)
    lengths = lengths.at[(full_index + 1) % SEQS].set(short_value)
    return lengths.at[full_index].set(SLOT).astype(jnp.int32)


def plant(entries, stream_key, low, top_value):
    dims = entries.shape
    index_at = [jax.random.randint(jax.random.fold_in(stream_key, axis), (), 0, dims[axis]) for axis in range(len(dims))]
    entries = entries.at[tuple(index_at)].set(low)
    longest = dims.index(max(dims))
    index_at[longest] = (index_at[longest] + 1) % dims[longest]
    return entries.at[tuple(index_at)].set(top_value)


def shard_levels(rng, shape, pieces, least, top_value):
    loudness = 1.0
    for dim, shards_of in pieces:
        heights = jax.random.uniform(jax.random.fold_in(jax.random.fold_in(rng, 6), dim), (shards_of,), jnp.float32, least / len(pieces), top_value / len(pieces))
        loudness = loudness * jnp.repeat(jnp.exp(heights), shape[dim] // shards_of).reshape((-1,) + (1,) * (len(shape) - 1 - dim))
    return loudness


def bell_draw(own_key, extent, spread, limit, shards=(), held_as=jnp.bfloat16):
    array = jax.random.normal(own_key, extent, jnp.float32) * spread
    if len(shards) > 0:
        array = shard_levels(own_key, extent, shards, -0.22, 0.18) * array
    return jnp.clip(array, min=-limit, max=limit).astype(held_as)


def setup_inputs(seed: int = 0) -> dict:
    streams_of = jax.random.split(jax.random.key(seed), 9)
    prefix_tokens = bell_draw(streams_of[0], (TOKENS, MODEL_WIDTH), 1.0, 6.0, ((0, 16),))
    key_value_weight = bell_draw(streams_of[1], (MODEL_WIDTH, 2 * KEY_VALUE_HEADS * HEAD_SIZE), MODEL_WIDTH ** -0.5, 0.0625, ((0, 16), (1, 2)))
    prefix_lengths = draw_prefix_lengths(jax.random.fold_in(streams_of[8], 71), 0)
    start_offsets = plant(jax.random.randint(streams_of[3], (SEQS,), 0, CACHE_LENGTH - SLOT + 1), jax.random.fold_in(streams_of[3], 1), 0, CACHE_LENGTH - SLOT).astype(jnp.int32)
    queries = draw_queries(jax.random.fold_in(streams_of[8], 71), 0)
    key_value_cache = draw_key_value_cache(jax.random.fold_in(streams_of[8], 71), 0)
    cache_lengths = draw_cache_lengths(jax.random.fold_in(streams_of[8], 71), 0)
    out_weight = bell_draw(streams_of[7], (QUERY_HEADS * HEAD_SIZE, MODEL_WIDTH), (QUERY_HEADS * HEAD_SIZE // 64) ** -0.5, 0.5, ((0, 2), (1, 16)))
    return {"prefix_tokens": prefix_tokens, "key_value_weight": key_value_weight, "prefix_lengths": prefix_lengths, "start_offsets": start_offsets, "queries": queries, "key_value_cache": key_value_cache, "cache_lengths": cache_lengths, "out_weight": out_weight}


rope_base = 500000.0
masked_score = -1e30


def rotate_and_mask(projected, first_column, prefix_lengths, start_offsets):
    tok_rows, columns = projected.shape
    slot_index = jnp.arange(SLOT, dtype=jnp.int32)
    positions = (start_offsets[:, None] + slot_index[None, :]).reshape(tok_rows)
    live_rows = (slot_index[None, :] < prefix_lengths[:, None]).reshape(tok_rows)
    half_width = HEAD_SIZE // 2
    freq_index = jnp.arange(half_width, dtype=jnp.float32)
    inverse = rope_base ** (-2.0 * freq_index / HEAD_SIZE)
    angles = positions.astype(jnp.float32)[:, None] * inverse[None, :]
    cosine = jnp.cos(angles)[:, None, :]
    sine = jnp.sin(angles)[:, None, :]
    head_list = projected.reshape(tok_rows, columns // HEAD_SIZE, HEAD_SIZE)
    first_half = head_list[:, :, :half_width]
    second_half = head_list[:, :, half_width:]
    rotary_applied = jnp.concatenate([first_half * cosine - second_half * sine, second_half * cosine + first_half * sine], axis=2)
    head_position = first_column // HEAD_SIZE + jnp.arange(columns // HEAD_SIZE, dtype=jnp.int32)
    key_tagged = jnp.where((head_position < KEY_VALUE_HEADS)[None, :, None], rotary_applied, head_list)
    kept = jnp.where(live_rows[:, None, None], key_tagged, 0.0)
    return kept.reshape(tok_rows, columns).astype(jnp.bfloat16)


def attend_one(query_vector, cache_entry_row, length):
    query_group = QUERY_HEADS // KEY_VALUE_HEADS
    query_head_rows = query_vector.astype(jnp.float32).reshape(KEY_VALUE_HEADS, query_group, HEAD_SIZE)
    key_rows = cache_entry_row[0].astype(jnp.float32).reshape(N_GX, CACHE_PER_SHARD, KEY_VALUE_HEADS, HEAD_SIZE)
    value_rows = cache_entry_row[1].astype(jnp.float32).reshape(N_GX, CACHE_PER_SHARD, KEY_VALUE_HEADS, HEAD_SIZE)
    scores = jnp.einsum("hgd,kphd->khgp", query_head_rows, key_rows, precision=lax.Precision.HIGHEST) * (HEAD_SIZE ** -0.5)
    position = jnp.arange(CACHE_LENGTH, dtype=jnp.int32).reshape(N_GX, 1, 1, CACHE_PER_SHARD)
    valid = position < length
    peak = jnp.max(jnp.where(valid, scores, masked_score), axis=3)
    weights = jnp.where(valid, jnp.exp(scores - peak[..., None]), 0.0)
    block_total = jnp.sum(weights, axis=3)
    rounded = lax.optimization_barrier(weights.astype(jnp.bfloat16)).astype(jnp.float32)
    numerator = jnp.einsum("khgp,kphd->khgd", rounded, value_rows, precision=lax.Precision.HIGHEST)
    highest = jnp.max(peak, axis=0)
    factor = jnp.exp(peak - highest[None])
    denominator = jnp.sum(block_total * factor, axis=0)
    combined = jnp.sum(numerator * factor[..., None], axis=0)
    return (combined / denominator[..., None]).reshape(QUERY_HEADS * HEAD_SIZE).astype(jnp.bfloat16)


def reference(prefix_tokens, key_value_weight, prefix_lengths, start_offsets, queries, key_value_cache, cache_lengths, out_weight):
    projected = jnp.dot(prefix_tokens, key_value_weight, preferred_element_type=jnp.float32)
    prefix_kv = rotate_and_mask(projected, 0, prefix_lengths, start_offsets)

    def one_trajectory(index):
        cache_entry_row = lax.dynamic_index_in_dim(key_value_cache, index, 1, keepdims=False)
        return attend_one(queries[index], cache_entry_row, cache_lengths[index])

    attention = lax.map(one_trajectory, jnp.arange(TRAJECTORY_COUNT, dtype=jnp.int32))
    decode_out = jnp.dot(attention, out_weight, preferred_element_type=jnp.float32).astype(jnp.bfloat16)
    return prefix_kv, decode_out
```

```python
import functools

import jax
import jax.numpy as jnp
from jax import lax
from jax.experimental import pallas as pl
from jax.experimental.pallas import tpu as pltpu
from jax.sharding import PartitionSpec as P

QUERY_HEADS = 64
KEY_VALUE_HEADS = 8
HEAD_SIZE = 128
SLOT = 128
MESH = pl.DeviceIdType.MESH


rope_base = 500000.0
masked_score = -1e30


def merged(part, axis, combine):
    gathered = jax.tree.map(lambda a: lax.all_gather(a, axis), part)

    def take(source):
        return jax.tree.map(lambda a: lax.dynamic_index_in_dim(a, source, 0, False), gathered)

    return lax.fori_loop(
        1, lax.axis_size(axis), lambda source, state: combine(state, take(source)), take(0)
    )


def plane_of(mesh):
    n = mesh.shape["gx"]
    line = list(mesh.devices[:, 0])
    where = [tuple(getattr(d, "coords", (i, 0, i))) for i, d in enumerate(line)]
    nc = 1
    while nc < n and where[nc] == where[0]:
        nc += 1
    row = 1
    while row < n and where[row][2] == where[0][2]:
        row += 1
    if row % nc or n % row:
        return n, 1, 1
    return n // row, row // nc, nc


def prefill_kernel(
    plane, groups, direct, x_hbm, w_hbm, cos_ref, sin_ref, mask_ref, o_ref,
    xbuf, wbuf, x_sem, own_sem, recv_sem, up_sem, down_sem, cross_sem, core_sem,
):
    nz, nx, nc = plane
    me = lax.axis_index("gx")
    key_groups = KEY_VALUE_HEADS - lax.axis_index("gy") * groups
    z = lax.div(me, nx * nc)
    x = lax.rem(lax.div(me, nc), nx)
    c = lax.rem(me, nc)
    depth = w_hbm.shape[0]
    rows = x_hbm.shape[0]
    tile = 256
    tiles = rows // tile
    travelled = groups - direct

    def index(zz, xx, cc):
        return (zz * nx + xx) * nc + cc

    def piece(g, block):
        return wbuf.at[g, pl.ds(pl.multiple_of(block * depth, depth), depth), :]

    def remote(g, block, sem, target):
        return pltpu.make_async_remote_copy(
            src_ref=piece(g, block), dst_ref=piece(g, block), send_sem=sem,
            recv_sem=recv_sem.at[g, block], device_id={"gx": target}, device_id_type=MESH,
        )

    def arrived(g, block):
        remote(g, block, up_sem.at[0, 0], me).wait_recv()

    def plane_block(block):
        return lax.div(block, nc)

    def send_up(g, block, act):
        @pl.when(z < nz - 1)
        def _():
            act(remote(g, block, up_sem.at[g, plane_block(block)], index(z + 1, x, c)))

    def send_down(g, block, act):
        @pl.when(z > 0)
        def _():
            act(remote(g, block, down_sem.at[g, plane_block(block)], index(z - 1, x, c)))

    def send_cross(g, block, act):
        for step in range(1, nx):
            act(remote(g, block, cross_sem.at[g, plane_block(block), step - 1], index(z, lax.rem(x + step, nx), c)))

    def send_core(g, block, act):
        for step in range(1, nc):
            act(remote(g, block, core_sem.at[g, plane_block(block), step - 1], index(z, x, lax.rem(c + step, nc))))

    start = lambda copy: copy.start()
    finish = lambda copy: copy.wait_send()

    def own_copy(g):
        return pltpu.make_async_copy(w_hbm.at[:, pl.ds(pl.multiple_of(g * HEAD_SIZE, HEAD_SIZE), HEAD_SIZE)], piece(g, me), own_sem.at[g])

    def each(low, high, body):
        lax.fori_loop(low, high, lambda i, s: (body(i), s)[1], 0)

    x_copy = pltpu.make_async_copy(x_hbm, xbuf, x_sem)
    if direct:
        own_copy(groups - 1).start()
    each(0, travelled, lambda g: own_copy(g).start())
    x_copy.start()

    barrier = pltpu.get_barrier_semaphore()

    def greet(target):
        pl.semaphore_signal(barrier, inc=1, device_id={"gx": target}, device_id_type=MESH)

    @pl.when(z > 0)
    def _():
        greet(index(z - 1, x, c))

    @pl.when(z < nz - 1)
    def _():
        greet(index(z + 1, x, c))

    for step in range(1, nx):
        greet(index(z, lax.rem(x + step, nx), c))
    for step in range(1, nc):
        greet(index(z, x, lax.rem(c + step, nc)))

    peers = nx + nc - 2 + jnp.where(z > 0, 1, 0) + jnp.where(z < nz - 1, 1, 0)
    pl.semaphore_wait(barrier, peers)

    def send_own(g, act):
        send_up(g, me, act)
        send_down(g, me, act)
        send_cross(g, me, act)
        send_core(g, me, act)

    def ready_own(g):
        own_copy(g).wait()
        send_own(g, start)

    last = groups - 1
    ahead = min(2, travelled)
    ready_own(jnp.int32(0))
    if direct:
        ready_own(jnp.int32(last))
    each(1, ahead, ready_own)

    def from_z(g, zs, xs, crossing, act):
        block = index(zs, xs, c)

        @pl.when(zs < z)
        def _():
            send_up(g, block, act)

        @pl.when(zs > z)
        def _():
            send_down(g, block, act)

        if crossing:
            send_cross(g, block, act)
        send_core(g, block, act)

    def both_sides(d, body):
        @pl.when(z >= d)
        def _():
            body(z - d)

        @pl.when(z + d < nz)
        def _():
            body(z + d)

    def take_z(g, d):
        def side(zs):
            arrived(g, index(zs, x, c))
            from_z(g, zs, x, True, start)

        both_sides(d, side)

    def take_x(g):
        for step in range(1, nx):
            def one(zs, step=step):
                block = index(zs, lax.rem(x + step, nx), c)
                arrived(g, block)
                send_core(g, block, start)

            each(0, nz, one)

    def take_core(g):
        for step in range(1, nc):
            def one(chip, step=step):
                arrived(g, chip * nc + lax.rem(c + step, nc))

            each(0, nz * nx, one)

    def direct_first(act, waiting):
        for step in range(1, nx):
            block = index(z, lax.rem(x + step, nx), c)
            if waiting:
                arrived(last, block)
            send_up(last, block, act)
            send_down(last, block, act)
            send_core(last, block, act)

    def direct_z(s, act, waiting):
        d = 1 + lax.div(s, nx)
        xs = lax.rem(x + lax.rem(s, nx), nx)

        def side(zs):
            if waiting:
                arrived(last, index(zs, xs, c))
            from_z(last, zs, xs, False, act)

        both_sides(d, side)

    def multiply(g, r):
        span = pl.ds(pl.multiple_of(r * tile, tile), tile)
        value = jnp.dot(xbuf[span, :], wbuf[g], preferred_element_type=jnp.float32)
        turned = value * cos_ref[span, :] + pltpu.roll(value, HEAD_SIZE // 2, 1) * sin_ref[span, :]
        value = jnp.where(g < key_groups, turned, value)
        value = jnp.where(mask_ref[span, :] > 0.0, value, 0.0)
        o_ref[span, pl.ds(pl.multiple_of(g * HEAD_SIZE, HEAD_SIZE), HEAD_SIZE)] = value.astype(o_ref.dtype)

    x_copy.wait()

    def step(g):
        @pl.when(g + ahead < travelled)
        def _():
            ready_own(g + ahead)

        @pl.when(g >= 2)
        def _():
            take_core(g - 2)

        if direct:
            @pl.when(g == 0)
            def _():
                direct_first(start, True)

        def hop(d):
            take_z(g, d)

            @pl.when(jnp.logical_and(g >= 2, d <= tiles))
            def _():
                multiply(g - 2, d - 1)

        each(1, nz, hop)

        @pl.when(g >= 2)
        def _():
            each(min(nz - 1, tiles), tiles, lambda r: multiply(g - 2, r))

        @pl.when(g >= 1)
        def _():
            take_x(g - 1)

        if direct:
            @pl.when(g < (nz - 1) * nx)
            def _():
                direct_z(g, start, True)

    each(0, travelled, step)

    def whole(g):
        take_core(g)
        each(0, tiles, lambda r: multiply(g, r))

    def finish_group(i):
        g = i

        @pl.when(i == travelled - 1)
        def _():
            take_x(i)

        whole(g)

    if direct:
        order_low = max(travelled - 2, 0)
        def closing(i):
            g = lax.rem(i + 1, 3)
            g = jnp.where(i == 0, last, order_low + i - 1)
            @pl.when(i == 2)
            def _():
                take_x(g)
            whole(g)
        each(0, 3, closing)
    else:
        each(max(travelled - 2, 0), travelled, finish_group)

    def sent(g):
        send_own(g, finish)

        def hop(d):
            both_sides(d, lambda zs: from_z(g, zs, x, True, finish))

        each(1, nz, hop)
        for step in range(1, nx):
            each(0, nz, lambda zs, step=step: send_core(g, index(zs, lax.rem(x + step, nx), c), finish))

    each(0, travelled, sent)
    if direct:
        send_own(last, finish)
        direct_first(finish, False)
        each(0, (nz - 1) * nx, lambda s: direct_z(s, finish, False))


def prefill(plane, tokens, weight, prefix_lengths, start_offsets):
    nz, nx, nc = plane
    n = nz * nx * nc
    rows = tokens.shape[0]
    depth, columns = weight.shape
    groups = columns // HEAD_SIZE
    direct = 1 if groups >= 6 and nx > 1 and (nz - 1) * nx < groups else 0
    slot_index = jnp.arange(SLOT, dtype=jnp.int32)
    positions = (start_offsets[:, None] + slot_index[None, :]).reshape(rows)
    live = (slot_index[None, :] < prefix_lengths[:, None]).reshape(rows)
    half = HEAD_SIZE // 2
    inverse = rope_base ** (-2.0 * jnp.arange(half, dtype=jnp.float32) / HEAD_SIZE)
    angles = positions.astype(jnp.float32)[:, None] * inverse[None, :]
    cosine, sine = jnp.cos(angles), jnp.sin(angles)
    cosine = jnp.concatenate([cosine, cosine], axis=1)
    sine = jnp.concatenate([-sine, sine], axis=1)
    mask = jnp.broadcast_to(live[:, None], (rows, HEAD_SIZE)).astype(jnp.float32)
    chips = nz * nx
    vmem = pl.BlockSpec(memory_space=pltpu.VMEM)
    anywhere = pl.BlockSpec(memory_space=pl.ANY)
    dma = pltpu.SemaphoreType.DMA
    return pl.pallas_call(
        functools.partial(prefill_kernel, plane, groups, direct),
        out_shape=jax.ShapeDtypeStruct((rows, columns), jnp.bfloat16),
        in_specs=[anywhere, anywhere, vmem, vmem, vmem],
        out_specs=vmem,
        scratch_shapes=[
            pltpu.VMEM(tokens.shape, jnp.bfloat16),
            pltpu.VMEM((groups, n * depth, HEAD_SIZE), jnp.bfloat16),
            dma(()),
            dma((groups,)),
            dma((groups, n)),
            dma((groups, chips)),
            dma((groups, chips)),
            dma((groups, chips, max(nx - 1, 1))),
            dma((groups, chips, max(nc - 1, 1))),
        ],
        compiler_params=pltpu.CompilerParams(
            collective_id=0, has_side_effects=True, vmem_limit_bytes=48 * 1024 * 1024
        ),
        name="prefill",
    )(tokens, weight, cosine, sine, mask)


def merge_parts(earlier, later):
    highest = jnp.maximum(earlier[0], later[0])
    early_factor = jnp.exp(earlier[0] - highest)
    late_factor = jnp.exp(later[0] - highest)
    summed = earlier[1] * early_factor + later[1] * late_factor
    weighted = earlier[2] * early_factor[..., None] + later[2] * late_factor[..., None]
    return (highest, summed, weighted)


def shards(
    plane,
    prefix_tokens,
    key_value_weight,
    prefix_lengths,
    start_offsets,
    queries,
    key_value_cache,
    cache_lengths,
    out_weight,
):
    prefix_kv = prefill(plane, prefix_tokens, key_value_weight, prefix_lengths, start_offsets)
    trajectory_per_shard = queries.shape[0]
    cache_per_shard = key_value_cache.shape[2]
    query_group = QUERY_HEADS // KEY_VALUE_HEADS
    query_head_rows = queries.reshape(trajectory_per_shard, KEY_VALUE_HEADS, query_group, HEAD_SIZE)
    key_rows = key_value_cache[0].reshape(
        trajectory_per_shard, cache_per_shard, KEY_VALUE_HEADS, HEAD_SIZE
    )
    value_rows = key_value_cache[1].reshape(
        trajectory_per_shard, cache_per_shard, KEY_VALUE_HEADS, HEAD_SIZE
    )
    scores = jnp.einsum(
        "bhgd,bphd->bhgp", query_head_rows, key_rows, preferred_element_type=jnp.float32
    ) * HEAD_SIZE ** (-0.5)
    position = lax.axis_index("gx") * cache_per_shard + jnp.arange(cache_per_shard, dtype=jnp.int32)
    valid = (position[None, :] < cache_lengths[:, None])[:, None, None, :]
    peak = jnp.max(jnp.where(valid, scores, masked_score), axis=3)
    weights = jnp.where(valid, jnp.exp(scores - peak[..., None]), 0.0)
    block_total = jnp.sum(weights, axis=3)
    numerator = jnp.einsum(
        "bhgp,bphd->bhgd",
        weights.astype(jnp.bfloat16),
        value_rows,
        preferred_element_type=jnp.float32,
    )
    peak, block_total, numerator = merged((peak, block_total, numerator), "gx", merge_parts)
    attention = (
        (numerator / block_total[..., None])
        .reshape(trajectory_per_shard, QUERY_HEADS * HEAD_SIZE)
        .astype(jnp.bfloat16)
    )
    spread = lax.all_to_all(attention, "gy", split_axis=1, concat_axis=0, tiled=True)
    partial_value = jnp.dot(spread, out_weight, preferred_element_type=jnp.float32)
    whole = lax.psum(partial_value, "gy")
    mixed = lax.dynamic_slice_in_dim(
        whole, lax.axis_index("gy") * trajectory_per_shard, trajectory_per_shard, 0
    )
    return (prefix_kv, mixed.astype(jnp.bfloat16))


def solution(mesh):
    return jax.shard_map(
        functools.partial(shards, plane_of(mesh)),
        mesh=mesh,
        in_specs=(
            P("gx", None),
            P("gx", "gy"),
            P("gx"),
            P("gx"),
            P("gy", None),
            P(None, "gy", "gx", None),
            P("gy"),
            P("gy", "gx"),
        ),
        out_specs=(P("gx", "gy"), P("gy", "gx")),
        check_vma=False,
    )
```

```python
import functools

import jax
import jax.numpy as jnp
from jax import lax
from jax.experimental import pallas as pl
from jax.experimental.pallas import tpu as pltpu
from jax.sharding import PartitionSpec as P

QUERY_HEADS = 64
KEY_VALUE_HEADS = 8
HEAD_SIZE = 128
SLOT = 128
MESH = pl.DeviceIdType.MESH


rope_base = 500000.0
masked_score = -1e30


def plane_of(mesh):
    n = mesh.shape["gx"]
    line = list(mesh.devices[:, 0])
    where = [tuple(getattr(d, "coords", (i, 0, i))) for i, d in enumerate(line)]
    nc = 1
    while nc < n and where[nc] == where[0]:
        nc += 1
    row = 1
    while row < n and where[row][2] == where[0][2]:
        row += 1
    if row % nc or n % row:
        return n, 1, 1
    return n // row, row // nc, nc


def prefill_kernel(
    plane, groups, direct, x_hbm, w_hbm, cos_ref, sin_ref, mask_ref, o_ref,
    xbuf, wbuf, x_sem, own_sem, recv_sem, up_sem, down_sem, cross_sem, core_sem,
):
    nz, nx, nc = plane
    me = lax.axis_index("gx")
    key_groups = KEY_VALUE_HEADS - lax.axis_index("gy") * groups
    z = lax.div(me, nx * nc)
    x = lax.rem(lax.div(me, nc), nx)
    c = lax.rem(me, nc)
    depth = w_hbm.shape[0]
    rows = x_hbm.shape[0]
    tile = 256
    tiles = rows // tile
    travelled = groups - direct

    def index(zz, xx, cc):
        return (zz * nx + xx) * nc + cc

    def piece(g, block):
        return wbuf.at[g, pl.ds(pl.multiple_of(block * depth, depth), depth), :]

    def remote(g, block, sem, target):
        return pltpu.make_async_remote_copy(
            src_ref=piece(g, block), dst_ref=piece(g, block), send_sem=sem,
            recv_sem=recv_sem.at[g, block], device_id={"gx": target}, device_id_type=MESH,
        )

    def arrived(g, block):
        remote(g, block, up_sem.at[0, 0], me).wait_recv()

    def plane_block(block):
        return lax.div(block, nc)

    def send_up(g, block, act):
        @pl.when(z < nz - 1)
        def _():
            act(remote(g, block, up_sem.at[g, plane_block(block)], index(z + 1, x, c)))

    def send_down(g, block, act):
        @pl.when(z > 0)
        def _():
            act(remote(g, block, down_sem.at[g, plane_block(block)], index(z - 1, x, c)))

    def send_cross(g, block, act):
        for step in range(1, nx):
            act(remote(g, block, cross_sem.at[g, plane_block(block), step - 1], index(z, lax.rem(x + step, nx), c)))

    def send_core(g, block, act):
        for step in range(1, nc):
            act(remote(g, block, core_sem.at[g, plane_block(block), step - 1], index(z, x, lax.rem(c + step, nc))))

    start = lambda copy: copy.start()
    finish = lambda copy: copy.wait_send()

    def own_copy(g):
        return pltpu.make_async_copy(w_hbm.at[:, pl.ds(pl.multiple_of(g * HEAD_SIZE, HEAD_SIZE), HEAD_SIZE)], piece(g, me), own_sem.at[g])

    def each(low, high, body):
        lax.fori_loop(low, high, lambda i, s: (body(i), s)[1], 0)

    x_copy = pltpu.make_async_copy(x_hbm, xbuf, x_sem)
    if direct:
        own_copy(groups - 1).start()
    each(0, travelled, lambda g: own_copy(g).start())
    x_copy.start()

    barrier = pltpu.get_barrier_semaphore()

    def greet(target):
        pl.semaphore_signal(barrier, inc=1, device_id={"gx": target}, device_id_type=MESH)

    @pl.when(z > 0)
    def _():
        greet(index(z - 1, x, c))

    @pl.when(z < nz - 1)
    def _():
        greet(index(z + 1, x, c))

    for step in range(1, nx):
        greet(index(z, lax.rem(x + step, nx), c))
    for step in range(1, nc):
        greet(index(z, x, lax.rem(c + step, nc)))

    peers = nx + nc - 2 + jnp.where(z > 0, 1, 0) + jnp.where(z < nz - 1, 1, 0)
    pl.semaphore_wait(barrier, peers)

    def send_own(g, act):
        send_up(g, me, act)
        send_down(g, me, act)
        send_cross(g, me, act)
        send_core(g, me, act)

    def ready_own(g):
        own_copy(g).wait()
        send_own(g, start)

    last = groups - 1
    ahead = min(2, travelled)
    ready_own(jnp.int32(0))
    if direct:
        ready_own(jnp.int32(last))
    each(1, ahead, ready_own)

    def from_z(g, zs, xs, crossing, act):
        block = index(zs, xs, c)

        @pl.when(zs < z)
        def _():
            send_up(g, block, act)

        @pl.when(zs > z)
        def _():
            send_down(g, block, act)

        if crossing:
            send_cross(g, block, act)
        send_core(g, block, act)

    def both_sides(d, body):
        @pl.when(z >= d)
        def _():
            body(z - d)

        @pl.when(z + d < nz)
        def _():
            body(z + d)

    def take_z(g, d):
        def side(zs):
            arrived(g, index(zs, x, c))
            from_z(g, zs, x, True, start)

        both_sides(d, side)

    def take_x(g):
        for step in range(1, nx):
            def one(zs, step=step):
                block = index(zs, lax.rem(x + step, nx), c)
                arrived(g, block)
                send_core(g, block, start)

            each(0, nz, one)

    def take_core(g):
        for step in range(1, nc):
            def one(chip, step=step):
                arrived(g, chip * nc + lax.rem(c + step, nc))

            each(0, nz * nx, one)

    def direct_first(act, waiting):
        for step in range(1, nx):
            block = index(z, lax.rem(x + step, nx), c)
            if waiting:
                arrived(last, block)
            send_up(last, block, act)
            send_down(last, block, act)
            send_core(last, block, act)

    def direct_z(s, act, waiting):
        d = 1 + lax.div(s, nx)
        xs = lax.rem(x + lax.rem(s, nx), nx)

        def side(zs):
            if waiting:
                arrived(last, index(zs, xs, c))
            from_z(last, zs, xs, False, act)

        both_sides(d, side)

    def multiply(g, r):
        span = pl.ds(pl.multiple_of(r * tile, tile), tile)
        value = jnp.dot(xbuf[span, :], wbuf[g], preferred_element_type=jnp.float32)
        turned = value * cos_ref[span, :] + pltpu.roll(value, HEAD_SIZE // 2, 1) * sin_ref[span, :]
        value = jnp.where(g < key_groups, turned, value)
        value = jnp.where(mask_ref[span, :] > 0.0, value, 0.0)
        o_ref[span, pl.ds(pl.multiple_of(g * HEAD_SIZE, HEAD_SIZE), HEAD_SIZE)] = value.astype(o_ref.dtype)

    x_copy.wait()

    def step(g):
        @pl.when(g + ahead < travelled)
        def _():
            ready_own(g + ahead)

        @pl.when(g >= 2)
        def _():
            take_core(g - 2)

        if direct:
            @pl.when(g == 0)
            def _():
                direct_first(start, True)

        def hop(d):
            take_z(g, d)

            @pl.when(jnp.logical_and(g >= 2, d <= tiles))
            def _():
                multiply(g - 2, d - 1)

        each(1, nz, hop)

        @pl.when(g >= 2)
        def _():
            each(min(nz - 1, tiles), tiles, lambda r: multiply(g - 2, r))

        @pl.when(g >= 1)
        def _():
            take_x(g - 1)

        if direct:
            @pl.when(g < (nz - 1) * nx)
            def _():
                direct_z(g, start, True)

    each(0, travelled, step)

    def whole(g):
        take_core(g)
        each(0, tiles, lambda r: multiply(g, r))

    def finish_group(i):
        g = i

        @pl.when(i == travelled - 1)
        def _():
            take_x(i)

        whole(g)

    if direct:
        order_low = max(travelled - 2, 0)
        def closing(i):
            g = lax.rem(i + 1, 3)
            g = jnp.where(i == 0, last, order_low + i - 1)
            @pl.when(i == 2)
            def _():
                take_x(g)
            whole(g)
        each(0, 3, closing)
    else:
        each(max(travelled - 2, 0), travelled, finish_group)

    def sent(g):
        send_own(g, finish)

        def hop(d):
            both_sides(d, lambda zs: from_z(g, zs, x, True, finish))

        each(1, nz, hop)
        for step in range(1, nx):
            each(0, nz, lambda zs, step=step: send_core(g, index(zs, lax.rem(x + step, nx), c), finish))

    each(0, travelled, sent)
    if direct:
        send_own(last, finish)
        direct_first(finish, False)
        each(0, (nz - 1) * nx, lambda s: direct_z(s, finish, False))


def prefill(plane, tokens, weight, prefix_lengths, start_offsets):
    nz, nx, nc = plane
    n = nz * nx * nc
    rows = tokens.shape[0]
    depth, columns = weight.shape
    groups = columns // HEAD_SIZE
    direct = 1 if groups >= 6 and nx > 1 and (nz - 1) * nx < groups else 0
    slot_index = jnp.arange(SLOT, dtype=jnp.int32)
    positions = (start_offsets[:, None] + slot_index[None, :]).reshape(rows)
    live = (slot_index[None, :] < prefix_lengths[:, None]).reshape(rows)
    half = HEAD_SIZE // 2
    inverse = rope_base ** (-2.0 * jnp.arange(half, dtype=jnp.float32) / HEAD_SIZE)
    angles = positions.astype(jnp.float32)[:, None] * inverse[None, :]
    cosine, sine = jnp.cos(angles), jnp.sin(angles)
    cosine = jnp.concatenate([cosine, cosine], axis=1)
    sine = jnp.concatenate([-sine, sine], axis=1)
    mask = jnp.broadcast_to(live[:, None], (rows, HEAD_SIZE)).astype(jnp.float32)
    chips = nz * nx
    vmem = pl.BlockSpec(memory_space=pltpu.VMEM)
    anywhere = pl.BlockSpec(memory_space=pl.ANY)
    dma = pltpu.SemaphoreType.DMA
    return pl.pallas_call(
        functools.partial(prefill_kernel, plane, groups, direct),
        out_shape=jax.ShapeDtypeStruct((rows, columns), jnp.bfloat16),
        in_specs=[anywhere, anywhere, vmem, vmem, vmem],
        out_specs=vmem,
        scratch_shapes=[
            pltpu.VMEM(tokens.shape, jnp.bfloat16),
            pltpu.VMEM((groups, n * depth, HEAD_SIZE), jnp.bfloat16),
            dma(()),
            dma((groups,)),
            dma((groups, n)),
            dma((groups, chips)),
            dma((groups, chips)),
            dma((groups, chips, max(nx - 1, 1))),
            dma((groups, chips, max(nc - 1, 1))),
        ],
        compiler_params=pltpu.CompilerParams(
            collective_id=0, has_side_effects=True, vmem_limit_bytes=48 * 1024 * 1024
        ),
        name="prefill",
    )(tokens, weight, cosine, sine, mask)


def decode_kernel(
    sizes, part_ref, w_hbm, o_ref,
    got, mine, spread, laid, wbuf, terms, red,
    w_sem, send1, recv1, send2, recv2, send3, recv3,
):
    n, lanes, batch, heads, near = sizes
    me = lax.axis_index("gx")
    side = lax.axis_index("gy")
    rows = batch * heads
    per_side = near // heads
    home = lax.div(me, per_side)
    slot = lax.rem(me, per_side)

    def each(low, high, body):
        lax.fori_loop(low, high, lambda i, s: (body(i), s)[1], 0)

    load = pltpu.make_async_copy(w_hbm, wbuf, w_sem)
    load.start()

    def scatter(step):
        to = lax.rem(me + step, n)
        return pltpu.make_async_remote_copy(
            src_ref=part_ref.at[to], dst_ref=got.at[me], send_sem=send1.at[step],
            recv_sem=recv1.at[me], device_id={"gx": to}, device_id_type=MESH,
        )

    def scattered(source):
        return pltpu.make_async_remote_copy(
            src_ref=part_ref.at[0], dst_ref=got.at[source], send_sem=send1.at[0],
            recv_sem=recv1.at[source], device_id={"gx": source}, device_id_type=MESH,
        )

    each(1, n, lambda step: scatter(step).start())
    got[me] = part_ref[me]
    each(1, n, lambda step: scattered(lax.rem(me + step, n)).wait_recv())
    top = lax.fori_loop(
        0, n, lambda i, t: jnp.maximum(t, got[i, rows : 2 * rows, :]), jnp.full((rows, HEAD_SIZE), masked_score)
    )

    def add(i, state):
        total, combined = state
        factor = jnp.exp(got[i, rows : 2 * rows, :] - top)
        return total + got[i, 2 * rows :, :] * factor, combined + got[i, :rows, :] * factor

    nothing = jnp.zeros((rows, HEAD_SIZE), jnp.float32)
    total, combined = lax.fori_loop(0, n, add, (nothing, nothing))
    attention = (combined / total).astype(jnp.bfloat16).astype(jnp.float32)
    mine[...] = attention

    def hand(to):
        return pltpu.make_async_remote_copy(
            src_ref=mine, dst_ref=spread.at[side, slot], send_sem=send2.at[to],
            recv_sem=recv2.at[side, slot], device_id={"gx": to, "gy": home}, device_id_type=MESH,
        )

    def others(act):
        def one(step):
            to = lax.rem(me + step, n)

            @pl.when(jnp.logical_or(step > 0, home != side))
            def _():
                act(hand(to))

        each(0, n, one)

    others(lambda copy: copy.start())

    @pl.when(home == side)
    def _():
        spread[side, slot] = attention

    def take(i):
        s, j = lax.div(i, per_side), lax.rem(i, per_side)
        source = side * per_side + j

        @pl.when(jnp.logical_or(s != side, source != me))
        def _():
            pltpu.make_async_remote_copy(
                src_ref=mine, dst_ref=spread.at[s, j], send_sem=send2.at[0],
                recv_sem=recv2.at[s, j], device_id={"gx": source, "gy": s}, device_id_type=MESH,
            ).wait_recv()

    each(0, lanes * per_side, take)
    for s in range(lanes):
        for j in range(per_side):
            for b in range(batch):
                for k in range(heads):
                    at = (j * heads + k) * HEAD_SIZE
                    laid[s * batch + b : s * batch + b + 1, at : at + HEAD_SIZE] = spread[
                        s, j, b * heads + k : b * heads + k + 1, :
                    ]
    load.wait()
    partial_value = jnp.dot(
        laid[...].astype(jnp.bfloat16), wbuf[...], preferred_element_type=jnp.float32
    )
    for s in range(lanes):
        terms[s] = partial_value[s * batch : (s + 1) * batch, :]

    def give(step):
        to = lax.rem(side + step, lanes)
        return pltpu.make_async_remote_copy(
            src_ref=terms.at[to], dst_ref=red.at[side], send_sem=send3.at[step],
            recv_sem=recv3.at[side], device_id={"gy": to}, device_id_type=MESH,
        )

    def given(step):
        source = lax.rem(side + step, lanes)
        return pltpu.make_async_remote_copy(
            src_ref=terms.at[0], dst_ref=red.at[source], send_sem=send3.at[0],
            recv_sem=recv3.at[source], device_id={"gy": source}, device_id_type=MESH,
        )

    each(1, lanes, lambda step: give(step).start())
    red[side] = terms[side]
    each(1, lanes, lambda step: given(step).wait_recv())
    whole = red[0]
    for s in range(1, lanes):
        whole = whole + red[s]
    o_ref[...] = whole.astype(o_ref.dtype)
    each(1, n, lambda step: scatter(step).wait_send())
    others(lambda copy: copy.wait_send())
    each(1, lanes, lambda step: give(step).wait_send())


def decode(sizes, peak, block_total, numerator, out_weight):
    n, lanes, batch, heads, near = sizes

    def by_owner(a):
        a = jnp.broadcast_to(a, (batch, KEY_VALUE_HEADS, QUERY_HEADS // KEY_VALUE_HEADS, HEAD_SIZE))
        a = a.reshape(batch, n, heads, HEAD_SIZE).transpose(1, 0, 2, 3)
        return a.reshape(n, batch * heads, HEAD_SIZE)

    parts = jnp.concatenate(
        [by_owner(numerator), by_owner(peak[..., None]), by_owner(block_total[..., None])], axis=1
    )
    rows = batch * heads
    depth, columns = out_weight.shape
    per_side = near // heads
    vmem = pl.BlockSpec(memory_space=pltpu.VMEM)
    dma = pltpu.SemaphoreType.DMA
    return pl.pallas_call(
        functools.partial(decode_kernel, sizes),
        out_shape=jax.ShapeDtypeStruct((batch, columns), jnp.bfloat16),
        in_specs=[vmem, pl.BlockSpec(memory_space=pl.ANY)],
        out_specs=vmem,
        scratch_shapes=[
            pltpu.VMEM((n, 3 * rows, HEAD_SIZE), jnp.float32),
            pltpu.VMEM((rows, HEAD_SIZE), jnp.float32),
            pltpu.VMEM((lanes, per_side, rows, HEAD_SIZE), jnp.float32),
            pltpu.VMEM((lanes * batch, depth), jnp.float32),
            pltpu.VMEM((depth, columns), jnp.bfloat16),
            pltpu.VMEM((lanes, batch, columns), jnp.float32),
            pltpu.VMEM((lanes, batch, columns), jnp.float32),
            dma(()),
            dma((n,)),
            dma((n,)),
            dma((n,)),
            dma((lanes, per_side)),
            dma((lanes,)),
            dma((lanes,)),
        ],
        compiler_params=pltpu.CompilerParams(
            has_side_effects=True, vmem_limit_bytes=24 * 1024 * 1024
        ),
        name="decode",
    )(parts, out_weight)


def shards(
    plane,
    prefix_tokens,
    key_value_weight,
    prefix_lengths,
    start_offsets,
    queries,
    key_value_cache,
    cache_lengths,
    out_weight,
):
    prefix_kv = prefill(plane, prefix_tokens, key_value_weight, prefix_lengths, start_offsets)
    trajectory_per_shard = queries.shape[0]
    cache_per_shard = key_value_cache.shape[2]
    query_group = QUERY_HEADS // KEY_VALUE_HEADS
    query_head_rows = queries.reshape(trajectory_per_shard, KEY_VALUE_HEADS, query_group, HEAD_SIZE)
    key_rows = key_value_cache[0].reshape(
        trajectory_per_shard, cache_per_shard, KEY_VALUE_HEADS, HEAD_SIZE
    )
    value_rows = key_value_cache[1].reshape(
        trajectory_per_shard, cache_per_shard, KEY_VALUE_HEADS, HEAD_SIZE
    )
    scores = jnp.einsum(
        "bhgd,bphd->bhgp", query_head_rows, key_rows, preferred_element_type=jnp.float32
    ) * HEAD_SIZE ** (-0.5)
    position = lax.axis_index("gx") * cache_per_shard + jnp.arange(cache_per_shard, dtype=jnp.int32)
    valid = (position[None, :] < cache_lengths[:, None])[:, None, None, :]
    peak = jnp.max(jnp.where(valid, scores, masked_score), axis=3)
    weights = jnp.where(valid, jnp.exp(scores - peak[..., None]), 0.0)
    block_total = jnp.sum(weights, axis=3)
    numerator = jnp.einsum(
        "bhgp,bphd->bhgd",
        weights.astype(jnp.bfloat16),
        value_rows,
        preferred_element_type=jnp.float32,
    )
    n = lax.axis_size("gx")
    sizes = (
        n, lax.axis_size("gy"), trajectory_per_shard, QUERY_HEADS // n, out_weight.shape[0] // HEAD_SIZE
    )
    decode_out = decode(sizes, peak, block_total, numerator, out_weight)
    return (prefix_kv, decode_out)


def solution(mesh):
    return jax.shard_map(
        functools.partial(shards, plane_of(mesh)),
        mesh=mesh,
        in_specs=(
            P("gx", None),
            P("gx", "gy"),
            P("gx"),
            P("gx"),
            P("gy", None),
            P(None, "gy", "gx", None),
            P("gy"),
            P("gy", "gx"),
        ),
        out_specs=(P("gx", "gy"), P("gy", "gx")),
        check_vma=False,
    )
```

```python
import functools

import jax
import jax.numpy as jnp
from jax import lax
from jax.experimental import pallas as pl
from jax.experimental.pallas import tpu as pltpu
from jax.sharding import PartitionSpec as P

QUERY_HEADS = 64
KEY_VALUE_HEADS = 8
HEAD_SIZE = 128
SLOT = 128
MESH = pl.DeviceIdType.MESH


rope_base = 500000.0
masked_score = -1e30


def plane_of(mesh):
    n = mesh.shape["gx"]
    line = list(mesh.devices[:, 0])
    where = [tuple(getattr(d, "coords", (i, 0, i))) for i, d in enumerate(line)]
    nc = 1
    while nc < n and where[nc] == where[0]:
        nc += 1
    row = 1
    while row < n and where[row][2] == where[0][2]:
        row += 1
    if row % nc or n % row:
        return n, 1, 1
    return n // row, row // nc, nc


def decode_phases(
    sizes, part_ref, w_hbm, o_ref,
    got, mine, spread, laid, wbuf, terms, red,
    w_sem, send1, recv1, send2, recv2, send3, recv3,
):
    n, lanes, batch, heads, near = sizes
    me = lax.axis_index("gx")
    side = lax.axis_index("gy")
    rows = batch * heads
    per_side = near // heads
    home = lax.div(me, per_side)
    slot = lax.rem(me, per_side)

    def each(low, high, body):
        lax.fori_loop(low, high, lambda i, s: (body(i), s)[1], 0)

    load = pltpu.make_async_copy(w_hbm, wbuf, w_sem)

    def scatter(step):
        to = lax.rem(me + step, n)
        return pltpu.make_async_remote_copy(
            src_ref=part_ref.at[to], dst_ref=got.at[me], send_sem=send1.at[step],
            recv_sem=recv1.at[me], device_id={"gx": to}, device_id_type=MESH,
        )

    def scattered(source):
        return pltpu.make_async_remote_copy(
            src_ref=part_ref.at[0], dst_ref=got.at[source], send_sem=send1.at[0],
            recv_sem=recv1.at[source], device_id={"gx": source}, device_id_type=MESH,
        )

    def begin():
        load.start()
        each(1, n, lambda step: scatter(step).start())

    def hand(to):
        return pltpu.make_async_remote_copy(
            src_ref=mine, dst_ref=spread.at[side, slot], send_sem=send2.at[to],
            recv_sem=recv2.at[side, slot], device_id={"gx": to, "gy": home}, device_id_type=MESH,
        )

    def others(act):
        def one(step):
            to = lax.rem(me + step, n)

            @pl.when(jnp.logical_or(step > 0, home != side))
            def _():
                act(hand(to))

        each(0, n, one)

    def merge():
        got[me] = part_ref[me]
        each(1, n, lambda step: scattered(lax.rem(me + step, n)).wait_recv())
        top = lax.fori_loop(
            0, n, lambda i, t: jnp.maximum(t, got[i, rows : 2 * rows, :]), jnp.full((rows, HEAD_SIZE), masked_score)
        )

        def add(i, state):
            total, combined = state
            factor = jnp.exp(got[i, rows : 2 * rows, :] - top)
            return total + got[i, 2 * rows :, :] * factor, combined + got[i, :rows, :] * factor

        nothing = jnp.zeros((rows, HEAD_SIZE), jnp.float32)
        total, combined = lax.fori_loop(0, n, add, (nothing, nothing))
        attention = (combined / total).astype(jnp.bfloat16).astype(jnp.float32)
        mine[...] = attention

        others(lambda copy: copy.start())

        @pl.when(home == side)
        def _():
            spread[side, slot] = attention

    def take(i):
        s, j = lax.div(i, per_side), lax.rem(i, per_side)
        source = side * per_side + j

        @pl.when(jnp.logical_or(s != side, source != me))
        def _():
            pltpu.make_async_remote_copy(
                src_ref=mine, dst_ref=spread.at[s, j], send_sem=send2.at[0],
                recv_sem=recv2.at[s, j], device_id={"gx": source, "gy": s}, device_id_type=MESH,
            ).wait_recv()

    def give(step):
        to = lax.rem(side + step, lanes)
        return pltpu.make_async_remote_copy(
            src_ref=terms.at[to], dst_ref=red.at[side], send_sem=send3.at[step],
            recv_sem=recv3.at[side], device_id={"gy": to}, device_id_type=MESH,
        )

    def given(step):
        source = lax.rem(side + step, lanes)
        return pltpu.make_async_remote_copy(
            src_ref=terms.at[0], dst_ref=red.at[source], send_sem=send3.at[0],
            recv_sem=recv3.at[source], device_id={"gy": source}, device_id_type=MESH,
        )

    def project():
        each(0, lanes * per_side, take)
        for s in range(lanes):
            for j in range(per_side):
                for b in range(batch):
                    for k in range(heads):
                        at = (j * heads + k) * HEAD_SIZE
                        laid[s * batch + b : s * batch + b + 1, at : at + HEAD_SIZE] = spread[
                            s, j, b * heads + k : b * heads + k + 1, :
                        ]
        load.wait()
        partial_value = jnp.dot(
            laid[...].astype(jnp.bfloat16), wbuf[...], preferred_element_type=jnp.float32
        )
        for s in range(lanes):
            terms[s] = partial_value[s * batch : (s + 1) * batch, :]
        each(1, lanes, lambda step: give(step).start())
        red[side] = terms[side]

    def end():
        each(1, lanes, lambda step: given(step).wait_recv())
        whole = red[0]
        for s in range(1, lanes):
            whole = whole + red[s]
        o_ref[...] = whole.astype(o_ref.dtype)

    def drain():
        each(1, n, lambda step: scatter(step).wait_send())
        others(lambda copy: copy.wait_send())
        each(1, lanes, lambda step: give(step).wait_send())

    return begin, merge, project, end, drain


def decode_parts(sizes, peak, block_total, numerator, out_weight):
    n, lanes, batch, heads, near = sizes

    def by_owner(a):
        a = jnp.broadcast_to(a, (batch, KEY_VALUE_HEADS, QUERY_HEADS // KEY_VALUE_HEADS, HEAD_SIZE))
        a = a.reshape(batch, n, heads, HEAD_SIZE).transpose(1, 0, 2, 3)
        return a.reshape(n, batch * heads, HEAD_SIZE)

    parts = jnp.concatenate(
        [by_owner(numerator), by_owner(peak[..., None]), by_owner(block_total[..., None])], axis=1
    )
    rows = batch * heads
    depth, columns = out_weight.shape
    per_side = near // heads
    dma = pltpu.SemaphoreType.DMA
    scratch = [
        pltpu.VMEM((n, 3 * rows, HEAD_SIZE), jnp.float32),
        pltpu.VMEM((rows, HEAD_SIZE), jnp.float32),
        pltpu.VMEM((lanes, per_side, rows, HEAD_SIZE), jnp.float32),
        pltpu.VMEM((lanes * batch, depth), jnp.float32),
        pltpu.VMEM((depth, columns), jnp.bfloat16),
        pltpu.VMEM((lanes, batch, columns), jnp.float32),
        pltpu.VMEM((lanes, batch, columns), jnp.float32),
        dma(()),
        dma((n,)),
        dma((n,)),
        dma((n,)),
        dma((lanes, per_side)),
        dma((lanes,)),
        dma((lanes,)),
    ]
    return parts, scratch


def layer_kernel(
    plane, sizes, groups, direct, x_hbm, w_hbm, cos_ref, sin_ref, mask_ref, part_ref, ow_hbm, o_ref, d_ref,
    xbuf, wbuf, x_sem, own_sem, recv_sem, up_sem, down_sem, cross_sem, core_sem, *decode_refs,
):
    begin, merge, project, end, drain = decode_phases(sizes, part_ref, ow_hbm, d_ref, *decode_refs)
    nz, nx, nc = plane
    me = lax.axis_index("gx")
    key_groups = KEY_VALUE_HEADS - lax.axis_index("gy") * groups
    z = lax.div(me, nx * nc)
    x = lax.rem(lax.div(me, nc), nx)
    c = lax.rem(me, nc)
    depth = w_hbm.shape[0]
    rows = x_hbm.shape[0]
    tile = 256
    tiles = rows // tile
    travelled = groups - direct

    def index(zz, xx, cc):
        return (zz * nx + xx) * nc + cc

    def piece(g, block):
        return wbuf.at[g, pl.ds(pl.multiple_of(block * depth, depth), depth), :]

    def remote(g, block, sem, target):
        return pltpu.make_async_remote_copy(
            src_ref=piece(g, block), dst_ref=piece(g, block), send_sem=sem,
            recv_sem=recv_sem.at[g, block], device_id={"gx": target}, device_id_type=MESH,
        )

    def arrived(g, block):
        remote(g, block, up_sem.at[0, 0], me).wait_recv()

    def plane_block(block):
        return lax.div(block, nc)

    def send_up(g, block, act):
        @pl.when(z < nz - 1)
        def _():
            act(remote(g, block, up_sem.at[g, plane_block(block)], index(z + 1, x, c)))

    def send_down(g, block, act):
        @pl.when(z > 0)
        def _():
            act(remote(g, block, down_sem.at[g, plane_block(block)], index(z - 1, x, c)))

    def send_cross(g, block, act):
        for step in range(1, nx):
            act(remote(g, block, cross_sem.at[g, plane_block(block), step - 1], index(z, lax.rem(x + step, nx), c)))

    def send_core(g, block, act):
        for step in range(1, nc):
            act(remote(g, block, core_sem.at[g, plane_block(block), step - 1], index(z, x, lax.rem(c + step, nc))))

    start = lambda copy: copy.start()
    finish = lambda copy: copy.wait_send()

    def own_copy(g):
        return pltpu.make_async_copy(w_hbm.at[:, pl.ds(pl.multiple_of(g * HEAD_SIZE, HEAD_SIZE), HEAD_SIZE)], piece(g, me), own_sem.at[g])

    def each(low, high, body):
        lax.fori_loop(low, high, lambda i, s: (body(i), s)[1], 0)

    x_copy = pltpu.make_async_copy(x_hbm, xbuf, x_sem)
    if direct:
        own_copy(groups - 1).start()
    each(0, travelled, lambda g: own_copy(g).start())
    x_copy.start()

    begin()

    def send_own(g, act):
        send_up(g, me, act)
        send_down(g, me, act)
        send_cross(g, me, act)
        send_core(g, me, act)

    def ready_own(g):
        own_copy(g).wait()
        send_own(g, start)

    last = groups - 1
    ahead = min(2, travelled)
    ready_own(jnp.int32(0))
    if direct:
        ready_own(jnp.int32(last))
    each(1, ahead, ready_own)

    def from_z(g, zs, xs, crossing, act):
        block = index(zs, xs, c)

        @pl.when(zs < z)
        def _():
            send_up(g, block, act)

        @pl.when(zs > z)
        def _():
            send_down(g, block, act)

        if crossing:
            send_cross(g, block, act)
        send_core(g, block, act)

    def both_sides(d, body):
        @pl.when(z >= d)
        def _():
            body(z - d)

        @pl.when(z + d < nz)
        def _():
            body(z + d)

    def take_z(g, d):
        def side(zs):
            arrived(g, index(zs, x, c))
            from_z(g, zs, x, True, start)

        both_sides(d, side)

    def take_x(g):
        for step in range(1, nx):
            def one(zs, step=step):
                block = index(zs, lax.rem(x + step, nx), c)
                arrived(g, block)
                send_core(g, block, start)

            each(0, nz, one)

    def take_core(g):
        for step in range(1, nc):
            def one(chip, step=step):
                arrived(g, chip * nc + lax.rem(c + step, nc))

            each(0, nz * nx, one)

    def direct_first(act, waiting):
        for step in range(1, nx):
            block = index(z, lax.rem(x + step, nx), c)
            if waiting:
                arrived(last, block)
            send_up(last, block, act)
            send_down(last, block, act)
            send_core(last, block, act)

    def direct_z(s, act, waiting):
        d = 1 + lax.div(s, nx)
        xs = lax.rem(x + lax.rem(s, nx), nx)

        def side(zs):
            if waiting:
                arrived(last, index(zs, xs, c))
            from_z(last, zs, xs, False, act)

        both_sides(d, side)

    def multiply(g, r):
        span = pl.ds(pl.multiple_of(r * tile, tile), tile)
        value = jnp.dot(xbuf[span, :], wbuf[g], preferred_element_type=jnp.float32)
        turned = value * cos_ref[span, :] + pltpu.roll(value, HEAD_SIZE // 2, 1) * sin_ref[span, :]
        value = jnp.where(g < key_groups, turned, value)
        value = jnp.where(mask_ref[span, :] > 0.0, value, 0.0)
        o_ref[span, pl.ds(pl.multiple_of(g * HEAD_SIZE, HEAD_SIZE), HEAD_SIZE)] = value.astype(o_ref.dtype)

    x_copy.wait()

    def step(g):
        if travelled > 5:
            pl.when(g == 1)(merge)
            pl.when(g == 3)(project)
            pl.when(g == 5)(end)

        @pl.when(g >= 2)
        def _():
            take_core(g - 2)

        if direct:
            @pl.when(g == 0)
            def _():
                direct_first(start, True)

        def hop(d):
            take_z(g, d)

            @pl.when(jnp.logical_and(g >= 2, d <= tiles))
            def _():
                multiply(g - 2, d - 1)

        each(1, nz, hop)

        @pl.when(g + ahead < travelled)
        def _():
            ready_own(g + ahead)

        if direct:
            @pl.when(g < (nz - 1) * nx)
            def _():
                direct_z(g, start, True)

        @pl.when(g >= 2)
        def _():
            each(min(nz - 1, tiles), tiles, lambda r: multiply(g - 2, r))

        @pl.when(g >= 1)
        def _():
            take_x(g - 1)

    each(0, travelled, step)
    if travelled <= 5:
        merge()
        project()
        end()

    def whole(g):
        take_core(g)
        each(0, tiles, lambda r: multiply(g, r))

    def finish_group(i):
        g = i

        @pl.when(i == travelled - 1)
        def _():
            take_x(i)

        whole(g)

    if direct:
        order_low = max(travelled - 2, 0)
        def closing(i):
            g = jnp.where(i == 0, last, order_low + i - 1)
            @pl.when(i == 2)
            def _():
                take_x(g)
            whole(g)
        each(0, 3, closing)
    else:
        each(max(travelled - 2, 0), travelled, finish_group)

    def sent(g):
        send_own(g, finish)

        def hop(d):
            both_sides(d, lambda zs: from_z(g, zs, x, True, finish))

        each(1, nz, hop)
        for step in range(1, nx):
            each(0, nz, lambda zs, step=step: send_core(g, index(zs, lax.rem(x + step, nx), c), finish))

    each(0, travelled, sent)
    if direct:
        send_own(last, finish)
        direct_first(finish, False)
        each(0, (nz - 1) * nx, lambda s: direct_z(s, finish, False))
    drain()


def layer(plane, sizes, tokens, weight, prefix_lengths, start_offsets, peak, block_total, numerator, out_weight):
    nz, nx, nc = plane
    n = nz * nx * nc
    rows = tokens.shape[0]
    depth, columns = weight.shape
    groups = columns // HEAD_SIZE
    direct = 1 if groups >= 6 and nx > 1 and (nz - 1) * nx < groups else 0
    slot_index = jnp.arange(SLOT, dtype=jnp.int32)
    positions = (start_offsets[:, None] + slot_index[None, :]).reshape(rows)
    live = (slot_index[None, :] < prefix_lengths[:, None]).reshape(rows)
    half = HEAD_SIZE // 2
    inverse = rope_base ** (-2.0 * jnp.arange(half, dtype=jnp.float32) / HEAD_SIZE)
    angles = positions.astype(jnp.float32)[:, None] * inverse[None, :]
    cosine, sine = jnp.cos(angles), jnp.sin(angles)
    cosine = jnp.concatenate([cosine, cosine], axis=1)
    sine = jnp.concatenate([-sine, sine], axis=1)
    mask = jnp.broadcast_to(live[:, None], (rows, HEAD_SIZE)).astype(jnp.float32)
    parts, decode_scratch = decode_parts(sizes, peak, block_total, numerator, out_weight)
    chips = nz * nx
    vmem = pl.BlockSpec(memory_space=pltpu.VMEM)
    anywhere = pl.BlockSpec(memory_space=pl.ANY)
    dma = pltpu.SemaphoreType.DMA
    return pl.pallas_call(
        functools.partial(layer_kernel, plane, sizes, groups, direct),
        out_shape=(
            jax.ShapeDtypeStruct((rows, columns), jnp.bfloat16),
            jax.ShapeDtypeStruct((sizes[2], out_weight.shape[1]), jnp.bfloat16),
        ),
        in_specs=[anywhere, anywhere, vmem, vmem, vmem, vmem, anywhere],
        out_specs=(vmem, vmem),
        scratch_shapes=[
            pltpu.VMEM(tokens.shape, jnp.bfloat16),
            pltpu.VMEM((groups, n * depth, HEAD_SIZE), jnp.bfloat16),
            dma(()),
            dma((groups,)),
            dma((groups, n)),
            dma((groups, chips)),
            dma((groups, chips)),
            dma((groups, chips, max(nx - 1, 1))),
            dma((groups, chips, max(nc - 1, 1))),
            *decode_scratch,
        ],
        compiler_params=pltpu.CompilerParams(
            has_side_effects=True, vmem_limit_bytes=48 * 1024 * 1024
        ),
        name="layer",
    )(tokens, weight, cosine, sine, mask, parts, out_weight)


def shards(
    plane,
    prefix_tokens,
    key_value_weight,
    prefix_lengths,
    start_offsets,
    queries,
    key_value_cache,
    cache_lengths,
    out_weight,
):
    trajectory_per_shard = queries.shape[0]
    cache_per_shard = key_value_cache.shape[2]
    query_group = QUERY_HEADS // KEY_VALUE_HEADS
    query_head_rows = queries.reshape(trajectory_per_shard, KEY_VALUE_HEADS, query_group, HEAD_SIZE)
    key_rows = key_value_cache[0].reshape(
        trajectory_per_shard, cache_per_shard, KEY_VALUE_HEADS, HEAD_SIZE
    )
    value_rows = key_value_cache[1].reshape(
        trajectory_per_shard, cache_per_shard, KEY_VALUE_HEADS, HEAD_SIZE
    )
    scores = jnp.einsum(
        "bhgd,bphd->bhgp", query_head_rows, key_rows, preferred_element_type=jnp.float32
    ) * HEAD_SIZE ** (-0.5)
    position = lax.axis_index("gx") * cache_per_shard + jnp.arange(cache_per_shard, dtype=jnp.int32)
    valid = (position[None, :] < cache_lengths[:, None])[:, None, None, :]
    peak = jnp.max(jnp.where(valid, scores, masked_score), axis=3)
    weights = jnp.where(valid, jnp.exp(scores - peak[..., None]), 0.0)
    block_total = jnp.sum(weights, axis=3)
    numerator = jnp.einsum(
        "bhgp,bphd->bhgd",
        weights.astype(jnp.bfloat16),
        value_rows,
        preferred_element_type=jnp.float32,
    )
    n = lax.axis_size("gx")
    sizes = (
        n, lax.axis_size("gy"), trajectory_per_shard, QUERY_HEADS // n, out_weight.shape[0] // HEAD_SIZE
    )
    return layer(
        plane, sizes, prefix_tokens, key_value_weight, prefix_lengths, start_offsets,
        peak, block_total, numerator, out_weight,
    )


def solution(mesh):
    return jax.shard_map(
        functools.partial(shards, plane_of(mesh)),
        mesh=mesh,
        in_specs=(
            P("gx", None),
            P("gx", "gy"),
            P("gx"),
            P("gx"),
            P("gy", None),
            P(None, "gy", "gx", None),
            P("gy"),
            P("gy", "gx"),
        ),
        out_specs=(P("gx", "gy"), P("gy", "gx")),
        check_vma=False,
    )
```
